768 devices in a mesh: aa: 12 (over z), ba: 64 (over y, x, core).
Axes of the slice: x: 4, y: 8, z: 12, core: 2. Of those that a mesh axis runs over, the one named last changes fastest.
Arguments:
- grad_out: bfloat16 [98304, 4096], P('aa', 'ba')
- saved_input: bfloat16 [98304, 4096], P(('aa', 'ba'))
- keep_bits: int32 [98304, 128], P(('aa', 'ba')), may hold values from -2147483648 to 2147483647, as said below
- gain: float32 [4096], replicated, may hold values from 0.5 to 1.5
Outputs:
- grad_in: bfloat16 [98304, 4096], P(('aa', 'ba'))
- gain_grad: float32 [4096], P('ba')
The draws below stay inside these ranges and needn't reach their ends.
Inputs may be any that keep to these rules, and one draw needn't show every extreme that they name: `keep_bits`: bit k of word w in row t (bit 31 being the sign bit) is the keep flag of feature 32 * w + k of token t; about nine in ten flags are 1.
All inputs are finite; a program needn't handle non-finite values.
Results may differ from the reference program's by a relative error of at most 0.001.
Values may be sent and summed in bfloat16 or wider, within the bound.
No kernel may reach another device: no remote copies, remote signals or barrier semaphores. Data moves between devices by JAX's collectives and lax.ppermute only.
A program may use at most 32 MiB of HBM per device.

```python
import math
import jax
import jax.numpy as jnp
from jax import lax

D = 4096
TOKENS = 98304
WORDS = 128


def draw_grad_out(key, part):
    first = jax.random.fold_in(key, 11)
    second = jax.random.fold_in(key, 12)
    rise = 1.0 + 2.0 * jnp.arange(TOKENS, dtype=jnp.float32) / TOKENS
    rough = jnp.exp(jax.random.uniform(second, (TOKENS,), jnp.float32, jnp.log(0.5), jnp.log(2.0)))
    base = jax.random.normal(first, (TOKENS, D), jnp.float32)
    values = base * (rise * rough)[:, None]
    return values.astype(jnp.bfloat16)


def draw_saved_input(key, part):
    first = jax.random.fold_in(key, 21)
    second = jax.random.fold_in(key, 22)
    third = jax.random.fold_in(key, 23)
    base = jax.random.normal(first, (TOKENS, D), jnp.float32)
    row_scale = jnp.exp(jax.random.uniform(second, (TOKENS,), jnp.float32, jnp.log(0.3), jnp.log(3.0)))
    column_scale = jnp.exp(jax.random.uniform(third, (D,), jnp.float32, jnp.log(0.5), jnp.log(5.0)))
    values = base * row_scale[:, None] * column_scale[None, :]
    return values.astype(jnp.bfloat16)


def draw_keep_bits(key, part):
    picks = jax.random.randint(jax.random.fold_in(key, 31), (TOKENS, WORDS, 32), 0, 10)
    flags = (picks < 9).astype(jnp.int32)
    shifts = jnp.arange(32, dtype=jnp.int32)
    return jnp.sum(jnp.left_shift(flags, shifts[None, None, :]), axis=-1).astype(jnp.int32)


def setup_inputs(seed: int = 0) -> dict:
    seeds = jax.random.split(jax.random.key(seed), 5)
    grad_out = draw_grad_out(jax.random.fold_in(seeds[4], 71), 0)
    saved_input = draw_saved_input(jax.random.fold_in(seeds[4], 71), 0)
    keep_bits = draw_keep_bits(jax.random.fold_in(seeds[4], 71), 0)
    gain = jnp.clip(1.0 + 0.1 * jax.random.normal(seeds[3], (D,), jnp.float32), 0.5, 1.5)
    return {"grad_out": grad_out, "saved_input": saved_input, "keep_bits": keep_bits, "gain": gain}


KEEP_RATE = 0.9
EPSILON = 1e-06

def unpack_bits(words):
    shifts = jnp.arange(32, dtype=jnp.int32)
    bits = jnp.right_shift(words[:, :, None], shifts[None, None, :]) & 1
    return bits.reshape(words.shape[0], words.shape[1] * 32).astype(jnp.float32)

def rows_backward(grad_rows, input_rows, word_rows, gain):
    keep = unpack_bits(word_rows)
    dropped = input_rows.astype(jnp.float32) * keep * (1.0 / KEEP_RATE)
    inverse = lax.rsqrt(lax.optimization_barrier(jnp.mean(dropped * dropped, axis=-1, keepdims=True)) + EPSILON)
    normed = dropped * inverse
    grads = grad_rows.astype(jnp.float32)
    scaled = gain[None, :] * grads
    centre = lax.optimization_barrier(jnp.mean(scaled * normed, axis=-1, keepdims=True))
    grad_in = (inverse * (scaled - normed * centre) * keep * (1.0 / KEEP_RATE)).astype(jnp.bfloat16)
    partial_sum = lax.optimization_barrier(jnp.sum(grads * normed, axis=0))
    return (grad_in, partial_sum)

def reference(grad_out, saved_input, keep_bits, gain):
    block = math.gcd(TOKENS, 512)
    count = TOKENS // block

    def one_block(items):
        return rows_backward(items[0], items[1], items[2], gain)
    grad_in, partial_sums = lax.map(one_block, (grad_out.reshape(count, block, D), saved_input.reshape(count, block, D), keep_bits.reshape(count, block, WORDS)))
    gain_grad = lax.optimization_barrier(jnp.sum(partial_sums, axis=0)) * (1.0 / math.sqrt(TOKENS))
    return (grad_in.reshape(TOKENS, D), gain_grad)
```

```python
import math

import jax
import jax.numpy as jnp
from jax import lax
from jax.sharding import PartitionSpec as P

KEEP_RATE = 0.9
EPSILON = 1e-06
FIRST_BA = 36
FIRST_AA = 9


def rotated(devices, first):
    return [[(first + i) % devices for i in range(devices)]]


def roll(value, shift):
    return jnp.concatenate([value[shift:], value[:shift]], axis=0)


def exchange(parts, axis, first):
    devices = lax.axis_size(axis)
    arrived = lax.all_to_all(
        roll(parts, first), axis, 0, 0, tiled=True, axis_index_groups=rotated(devices, first)
    )
    return roll(arrived, devices - first)


def sum_over(parts, axis, first):
    devices = lax.axis_size(axis)
    arrived = lax.all_to_all(parts, axis, 0, 0, tiled=True, axis_index_groups=rotated(devices, first))
    return jnp.sum(arrived, axis=0)


def unpack_bits(words):
    shifts = jnp.arange(32, dtype=jnp.int32)
    bits = jnp.right_shift(words[:, :, None], shifts[None, None, :]) & 1
    return bits.reshape(words.shape[0], words.shape[1] * 32).astype(jnp.float32)


def rows_backward(grad_rows, input_rows, word_rows, gain):
    keep = unpack_bits(word_rows)
    dropped = input_rows.astype(jnp.float32) * keep * (1.0 / KEEP_RATE)
    inverse = lax.rsqrt(jnp.mean(dropped * dropped, axis=-1, keepdims=True) + EPSILON)
    normed = dropped * inverse
    grads = grad_rows.astype(jnp.float32)
    scaled = gain[None, :] * grads
    centre = jnp.mean(scaled * normed, axis=-1, keepdims=True)
    grad_in = (inverse * (scaled - normed * centre) * keep * (1.0 / KEEP_RATE)).astype(jnp.bfloat16)
    partial_sum = jnp.sum(grads * normed, axis=0)
    return (grad_in, partial_sum)


def per_device(grad_out, saved_input, keep_bits, gain):
    groups = lax.axis_size("ba")
    rows = grad_out.shape[0] // groups
    pieces = grad_out.reshape(groups, rows, grad_out.shape[1])
    arrived = exchange(pieces, "ba", FIRST_BA)
    grad_rows = jnp.moveaxis(arrived, 0, 1).reshape(rows, -1)
    grad_in, partial_sum = rows_backward(grad_rows, saved_input, keep_bits, gain)
    total_tokens = rows * groups * lax.axis_size("aa")
    owned = sum_over(roll(partial_sum.reshape(groups, -1), FIRST_BA), "ba", FIRST_BA)
    copies = jnp.broadcast_to(owned[None], (lax.axis_size("aa"), *owned.shape))
    share = sum_over(copies, "aa", FIRST_AA)
    gain_grad = share * (1.0 / math.sqrt(total_tokens))
    return (grad_in, gain_grad)


def solution(mesh):
    placed = (P("aa", "ba"), P(("aa", "ba"), None), P(("aa", "ba"), None), P())
    return jax.shard_map(
        per_device,
        mesh=mesh,
        in_specs=placed,
        out_specs=(P(("aa", "ba"), None), P("ba")),
        check_vma=False,
    )
```

```python
import functools
import math

import jax
import jax.numpy as jnp
from jax import lax
from jax.experimental import pallas as pl
from jax.experimental.pallas import tpu as pltpu
from jax.sharding import PartitionSpec as P

KEEP_RATE = 0.9
EPSILON = 1e-06
LANES = 128
BITS = 32
CHUNKS = 4
FIRST_BA = 36
FIRST_AA = 9
F32 = jnp.float32


def rotation(devices, first):
    return [(first + i) % devices for i in range(devices)]


def exchange(parts, axis, order):
    return lax.all_to_all(parts, axis, 0, 0, tiled=True, axis_index_groups=[order])


def params(mib):
    return pltpu.CompilerParams(vmem_limit_bytes=mib << 20)


def cost(flops, size):
    return pl.CostEstimate(flops=flops, bytes_accessed=size, transcendentals=0)


def arrange_kernel(order, grads, out, held, arrive, leave):
    devices, _, rows = out.shape
    each = devices // CHUNKS
    place = {device: i for i, device in enumerate(order)}

    def chunk(k):
        part = pl.ds(k * each * rows, each * rows)
        return pltpu.make_async_copy(grads.at[:, part], held.at[:, part], arrive.at[k])

    for k in range(CHUNKS):
        chunk(k).start()
    for k in range(CHUNKS):
        chunk(k).wait()
        for d in range(k * each, (k + 1) * each):
            piece = held.at[:, pl.ds(d * rows, rows)]
            pltpu.make_async_copy(piece, out.at[place[d]], leave).start()
    pltpu.make_async_copy(out, out, leave).wait()


def arrange(grads, order):
    features, tokens = grads.shape
    devices = len(order)
    return pl.pallas_call(
        functools.partial(arrange_kernel, order),
        out_shape=jax.ShapeDtypeStruct((devices, features, tokens // devices), grads.dtype),
        in_specs=[pl.BlockSpec(memory_space=pl.ANY)],
        out_specs=pl.BlockSpec(memory_space=pl.ANY),
        scratch_shapes=[
            pltpu.VMEM(grads.shape, grads.dtype),
            pltpu.SemaphoreType.DMA((CHUNKS,)),
            pltpu.SemaphoreType.DMA,
        ],
        cost_estimate=cost(10**6, 4 * grads.size),
        name="arrange",
    )(grads)


def keep_flags(words_t, q, rows):
    count = LANES // BITS
    shift = lax.broadcasted_iota(jnp.int32, (count, BITS, rows), 1)
    word = jnp.broadcast_to(words_t[q * count : (q + 1) * count, None, :], (count, BITS, rows))
    return (jnp.right_shift(word, shift) & 1).reshape(LANES, rows).astype(F32)


def unpack_kernel(order, inputs, words, by_device, scale):
    rows, width = inputs.shape
    features = width // len(order)
    words_t = words[...].T
    squares = jnp.zeros((8, rows), F32)
    place = {device: i for i, device in enumerate(order)}
    for q in range(width // LANES):
        at = slice(q * LANES, (q + 1) * LANES)
        value = inputs[:, at].astype(F32).T * keep_flags(words_t, q, rows)
        dropped = value * (1.0 / KEEP_RATE)
        squares += jnp.sum((dropped * dropped).reshape(LANES // 8, 8, rows), axis=0)
        for h in range(LANES // features):
            piece = value[h * features : (h + 1) * features, :]
            by_device[place[q * LANES // features + h]] = piece.astype(by_device.dtype)
    mean = jnp.sum(squares, axis=0, keepdims=True) * (1.0 / width)
    scale[...] = lax.rsqrt(mean + EPSILON) * (1.0 / KEEP_RATE)


def unpack(inputs, words, order):
    rows, width = inputs.shape
    devices = len(order)
    return pl.pallas_call(
        functools.partial(unpack_kernel, order),
        out_shape=(
            jax.ShapeDtypeStruct((devices, width // devices, rows), inputs.dtype),
            jax.ShapeDtypeStruct((1, rows), F32),
        ),
        compiler_params=params(6),
        cost_estimate=cost(10**8, 4 * inputs.size),
        name="unpack",
    )(inputs, words)


def token_sums_kernel(grads, inputs, scale, out):
    devices, features, rows = grads.shape
    shape = (features, LANES)
    diagonal = lax.broadcasted_iota(jnp.int32, shape, 0) == lax.broadcasted_iota(jnp.int32, shape, 1)
    for d in range(devices):
        product = grads[d].astype(F32) * (inputs[d].astype(F32) * scale[...])
        sums = jnp.sum(product, axis=1, keepdims=True)
        out[d : d + 1, :] = jnp.sum(jnp.where(diagonal, sums, 0.0), axis=0, keepdims=True)


def token_sums(grads, inputs, scale):
    return pl.pallas_call(
        token_sums_kernel,
        out_shape=jax.ShapeDtypeStruct((grads.shape[0], LANES), F32),
        compiler_params=params(6),
        cost_estimate=cost(10**7, 4 * grads.size),
        name="token_sums",
    )(grads, inputs, scale)


def input_grad_kernel(order, grads, inputs, words, scale, gain, out, scaled, normed, factor):
    rows, width = out.shape
    features = width // len(order)
    place = {device: i for i, device in enumerate(order)}
    words_t = words[...].T
    column = jnp.broadcast_to(scale[...], (LANES, rows)).T
    total = jnp.zeros((rows, LANES), F32)
    for q in range(width // LANES):
        at = slice(q * LANES, (q + 1) * LANES)
        parts = [grads[place[q * LANES // features + h]] for h in range(LANES // features)]
        value = jnp.concatenate(parts, axis=0).astype(F32).T * gain[:, at]
        kept = keep_flags(words_t, q, rows).T * column
        norm = inputs[:, at].astype(F32) * kept
        scaled[:, at] = value
        normed[:, at] = norm
        factor[:, at] = kept
        total += value * norm
    centre = jnp.sum(total, axis=1, keepdims=True) * (1.0 / width)
    for q in range(width // LANES):
        at = slice(q * LANES, (q + 1) * LANES)
        value = factor[:, at] * (scaled[:, at] - normed[:, at] * centre)
        out[:, at] = value.astype(out.dtype)


def input_grad(grads, inputs, words, scale, gain, order):
    rows, width = inputs.shape
    return pl.pallas_call(
        functools.partial(input_grad_kernel, order),
        out_shape=jax.ShapeDtypeStruct((rows, width), inputs.dtype),
        scratch_shapes=[pltpu.VMEM((rows, width), F32)] * 3,
        compiler_params=params(14),
        cost_estimate=cost(10**8, 8 * inputs.size),
        name="input_grad",
    )(grads, inputs, words, scale, gain.reshape(1, width))


def per_device(grad_out, saved_input, keep_bits, gain):
    groups, planes = lax.axis_size("ba"), lax.axis_size("aa")
    features = grad_out.shape[1]
    rows = saved_input.shape[0]
    order, order_aa = rotation(groups, FIRST_BA), rotation(planes, FIRST_AA)

    arrived = exchange(arrange(grad_out.T, order), "ba", order)
    by_device, scale = unpack(saved_input, keep_bits, order)
    partial_sum = token_sums(arrived, by_device, scale)
    owned = jnp.sum(exchange(partial_sum[:, None, :], "ba", order), axis=0)
    copies = jnp.broadcast_to(owned[None], (planes, *owned.shape))
    share = jnp.sum(exchange(copies, "aa", order_aa), axis=0).reshape(-1)[:features]
    gain_grad = share * (1.0 / math.sqrt(rows * groups * planes))

    late, _ = lax.optimization_barrier((arrived, owned))
    grad_in = input_grad(late, saved_input, keep_bits, scale, gain, order)
    return (grad_in, gain_grad)


def solution(mesh):
    placed = (P("aa", "ba"), P(("aa", "ba"), None), P(("aa", "ba"), None), P())
    return jax.shard_map(
        per_device,
        mesh=mesh,
        in_specs=placed,
        out_specs=(P(("aa", "ba"), None), P("ba")),
        check_vma=False,
    )
```

```python
import functools
import math

import jax
import jax.numpy as jnp
from jax import lax
from jax.experimental import pallas as pl
from jax.experimental.pallas import tpu as pltpu
from jax.sharding import PartitionSpec as P

KEEP_RATE = 0.9
EPSILON = 1e-06
LANES = 128
BITS = 32
FIRST_BA = 37
FIRST_AA = 9
F32 = jnp.float32


def rotation(devices, first):
    return [(first + i) % devices for i in range(devices)]


def exchange(parts, axis, order):
    return lax.all_to_all(parts, axis, 0, 0, tiled=True, axis_index_groups=[order])


def params(mib):
    return pltpu.CompilerParams(vmem_limit_bytes=mib << 20)


def cost(flops, size):
    return pl.CostEstimate(flops=flops, bytes_accessed=size, transcendentals=0)


def keep_flags(words_t, q, rows):
    count = LANES // BITS
    shift = lax.broadcasted_iota(jnp.int32, (count, BITS, rows), 1)
    word = jnp.broadcast_to(words_t[q * count : (q + 1) * count, None, :], (count, BITS, rows))
    return (jnp.right_shift(word, shift) & 1).reshape(LANES, rows).astype(F32)


def prepare_kernel(
    order, grads, inputs, words, pieces, by_device, scale, rows_in, words_in, kept, rows_sem, words_sem, move
):
    rows, width = inputs.shape
    features = width // len(order)
    place = {device: i for i, device in enumerate(order)}
    words_copy = pltpu.make_async_copy(words, words_in, words_sem)
    rows_copy = pltpu.make_async_copy(inputs, rows_in, rows_sem)
    words_copy.start()
    rows_copy.start()
    for i, device in enumerate(order):
        pltpu.make_async_copy(grads.at[:, pl.ds(device * rows, rows)], pieces.at[i], move).start()
    words_copy.wait()
    words_t = words_in[...].T
    for q in range(width // LANES):
        at = slice(q * LANES, (q + 1) * LANES)
        kept[at, :] = keep_flags(words_t, q, rows).astype(kept.dtype)
    rows_copy.wait()
    squares = jnp.zeros((8, rows), F32)
    for q in range(width // LANES):
        at = slice(q * LANES, (q + 1) * LANES)
        value = rows_in[:, at].T * kept[at, :]
        dropped = value.astype(F32) * (1.0 / KEEP_RATE)
        squares += jnp.sum((dropped * dropped).reshape(LANES // 8, 8, rows), axis=0)
        for h in range(LANES // features):
            by_device[place[q * LANES // features + h]] = value[h * features : (h + 1) * features, :]
    mean = jnp.sum(squares, axis=0, keepdims=True) * (1.0 / width)
    scale[...] = lax.rsqrt(mean + EPSILON) * (1.0 / KEEP_RATE)
    pltpu.make_async_copy(pieces, pieces, move).wait()


def prepare(grads, inputs, words, order):
    rows, width = inputs.shape
    devices = len(order)
    shape = (devices, width // devices, rows)
    return pl.pallas_call(
        functools.partial(prepare_kernel, order),
        out_shape=(
            jax.ShapeDtypeStruct(shape, grads.dtype),
            jax.ShapeDtypeStruct(shape, inputs.dtype),
            jax.ShapeDtypeStruct((1, rows), F32),
        ),
        in_specs=[pl.BlockSpec(memory_space=pltpu.HBM)] * 3,
        scratch_shapes=[
            pltpu.VMEM((rows, width), inputs.dtype),
            pltpu.VMEM(words.shape, words.dtype),
            pltpu.VMEM((width, rows), inputs.dtype),
            pltpu.SemaphoreType.DMA,
            pltpu.SemaphoreType.DMA,
            pltpu.SemaphoreType.DMA,
        ],
        compiler_params=params(6),
        cost_estimate=cost(10**8, 8 * inputs.size),
        name="prepare",
    )(*(pltpu.with_memory_space_constraint(value, pltpu.HBM) for value in (grads, inputs, words)))


def token_sums_kernel(grads, inputs, scale, out):
    devices, features, rows = grads.shape
    shape = (features, LANES)
    diagonal = lax.broadcasted_iota(jnp.int32, shape, 0) == lax.broadcasted_iota(jnp.int32, shape, 1)
    for d in range(devices):
        product = grads[d].astype(F32) * (inputs[d].astype(F32) * scale[...])
        sums = jnp.sum(product, axis=1, keepdims=True)
        out[d : d + 1, :] = jnp.sum(jnp.where(diagonal, sums, 0.0), axis=0, keepdims=True)


def token_sums(grads, inputs, scale):
    return pl.pallas_call(
        token_sums_kernel,
        out_shape=jax.ShapeDtypeStruct((grads.shape[0], LANES), F32),
        compiler_params=params(6),
        cost_estimate=cost(10**7, 4 * grads.size),
        name="token_sums",
    )(grads, inputs, scale)


def input_grad_kernel(order, grads, inputs, words, scale, gain, out, scaled, normed, factor):
    rows, width = out.shape
    features = width // len(order)
    place = {device: i for i, device in enumerate(order)}
    words_t = words[...].T
    column = jnp.broadcast_to(scale[...], (LANES, rows)).T
    total = jnp.zeros((rows, LANES), F32)
    for q in range(width // LANES):
        at = slice(q * LANES, (q + 1) * LANES)
        parts = [grads[place[q * LANES // features + h]] for h in range(LANES // features)]
        value = jnp.concatenate(parts, axis=0).astype(F32).T * gain[:, at]
        kept = keep_flags(words_t, q, rows).T * column
        norm = inputs[:, at].astype(F32) * kept
        scaled[:, at] = value
        normed[:, at] = norm
        factor[:, at] = kept
        total += value * norm
    centre = jnp.sum(total, axis=1, keepdims=True) * (1.0 / width)
    for q in range(width // LANES):
        at = slice(q * LANES, (q + 1) * LANES)
        value = factor[:, at] * (scaled[:, at] - normed[:, at] * centre)
        out[:, at] = value.astype(out.dtype)


def input_grad(grads, inputs, words, scale, gain, order):
    rows, width = inputs.shape
    return pl.pallas_call(
        functools.partial(input_grad_kernel, order),
        out_shape=jax.ShapeDtypeStruct((rows, width), inputs.dtype),
        scratch_shapes=[pltpu.VMEM((rows, width), F32)] * 3,
        compiler_params=params(14),
        cost_estimate=cost(10**8, 8 * inputs.size),
        name="input_grad",
    )(grads, inputs, words, scale, gain.reshape(1, width))


def per_device(grad_out, saved_input, keep_bits, gain):
    groups, planes = lax.axis_size("ba"), lax.axis_size("aa")
    features = grad_out.shape[1]
    rows = saved_input.shape[0]
    order, order_aa = rotation(groups, FIRST_BA), rotation(planes, FIRST_AA)

    pieces, by_device, scale = prepare(grad_out.T, saved_input, keep_bits, order)
    arrived = exchange(pieces, "ba", order)
    partial_sum = token_sums(arrived, by_device, scale)
    owned = jnp.sum(exchange(partial_sum[:, None, :], "ba", order), axis=0)
    copies = jnp.broadcast_to(owned[None], (planes, *owned.shape))
    share = jnp.sum(exchange(copies, "aa", order_aa), axis=0).reshape(-1)[:features]
    gain_grad = share * (1.0 / math.sqrt(rows * groups * planes))

    late, _ = lax.optimization_barrier((arrived, owned))
    grad_in = input_grad(late, saved_input, keep_bits, scale, gain, order)
    return (grad_in, gain_grad)


def solution(mesh):
    placed = (P("aa", "ba"), P(("aa", "ba"), None), P(("aa", "ba"), None), P())
    return jax.shard_map(
        per_device,
        mesh=mesh,
        in_specs=placed,
        out_specs=(P(("aa", "ba"), None), P("ba")),
        check_vma=False,
    )
```

```python
import functools
import math

import jax
import jax.numpy as jnp
from jax import lax
from jax.experimental import pallas as pl
from jax.experimental.pallas import tpu as pltpu
from jax.sharding import PartitionSpec as P

KEEP_RATE = 0.9
EPSILON = 1e-06
LANES = 128
BITS = 32
GRADS_ORDER = (37, 1)
SUMS_ORDER = (37, 1)
SHARES_ORDER = (9, 1)
EARLY = 4
F32 = jnp.float32


def members(devices, first, step):
    return [(first + i * step) % devices for i in range(devices)]


def exchange(parts, axis, order):
    return lax.all_to_all(parts, axis, 0, 0, tiled=True, axis_index_groups=[order])


def params(mib):
    return pltpu.CompilerParams(vmem_limit_bytes=mib << 20)


def cost(flops, size):
    return pl.CostEstimate(flops=flops, bytes_accessed=size, transcendentals=0)


def keep_flags(words_t, q, rows):
    count = LANES // BITS
    shift = lax.broadcasted_iota(jnp.int32, (count, BITS, rows), 1)
    word = jnp.broadcast_to(words_t[q * count : (q + 1) * count, None, :], (count, BITS, rows))
    return (jnp.right_shift(word, shift) & 1).reshape(LANES, rows).astype(F32)


def prepare_kernel(
    order, grads, inputs, words, pieces, by_device, scale, rows_in, words_in, kept, rows_sem, words_sem, move
):
    rows, width = inputs.shape
    features = width // len(order)
    place = {device: i for i, device in enumerate(order)}
    words_copy = pltpu.make_async_copy(words, words_in, words_sem)
    rows_copy = pltpu.make_async_copy(inputs, rows_in, rows_sem)
    words_copy.start()
    rows_copy.start()
    for i, device in enumerate(order):
        pltpu.make_async_copy(grads.at[:, pl.ds(device * rows, rows)], pieces.at[i], move).start()
    words_copy.wait()
    words_t = words_in[...].T
    for q in range(width // LANES):
        at = slice(q * LANES, (q + 1) * LANES)
        kept[at, :] = keep_flags(words_t, q, rows).astype(kept.dtype)
    rows_copy.wait()
    squares = jnp.zeros((8, rows), F32)
    for q in range(width // LANES):
        at = slice(q * LANES, (q + 1) * LANES)
        value = rows_in[:, at].T * kept[at, :]
        dropped = value.astype(F32) * (1.0 / KEEP_RATE)
        squares += jnp.sum((dropped * dropped).reshape(LANES // 8, 8, rows), axis=0)
        for h in range(LANES // features):
            by_device[place[q * LANES // features + h]] = value[h * features : (h + 1) * features, :]
    mean = jnp.sum(squares, axis=0, keepdims=True) * (1.0 / width)
    scale[...] = lax.rsqrt(mean + EPSILON) * (1.0 / KEEP_RATE)
    pltpu.make_async_copy(pieces, pieces, move).wait()


def prepare(grads, inputs, words, order):
    rows, width = inputs.shape
    devices = len(order)
    shape = (devices, width // devices, rows)
    return pl.pallas_call(
        functools.partial(prepare_kernel, order),
        out_shape=(
            jax.ShapeDtypeStruct(shape, grads.dtype),
            jax.ShapeDtypeStruct(shape, inputs.dtype),
            jax.ShapeDtypeStruct((1, rows), F32),
        ),
        in_specs=[pl.BlockSpec(memory_space=pltpu.HBM)] * 3,
        scratch_shapes=[
            pltpu.VMEM((rows, width), inputs.dtype),
            pltpu.VMEM(words.shape, words.dtype),
            pltpu.VMEM((width, rows), inputs.dtype),
            pltpu.SemaphoreType.DMA,
            pltpu.SemaphoreType.DMA,
            pltpu.SemaphoreType.DMA,
        ],
        compiler_params=params(6),
        cost_estimate=cost(10**8, 8 * inputs.size),
        name="prepare",
    )(*(pltpu.with_memory_space_constraint(value, pltpu.HBM) for value in (grads, inputs, words)))


def token_sums_kernel(order, out_order, grads, inputs, scale, out):
    devices, features, rows = grads.shape
    shape = (features, LANES)
    diagonal = lax.broadcasted_iota(jnp.int32, shape, 0) == lax.broadcasted_iota(jnp.int32, shape, 1)
    for d in range(devices):
        product = grads[d].astype(F32) * (inputs[d].astype(F32) * scale[...])
        sums = jnp.sum(product, axis=1, keepdims=True)
        row = out_order.index(order[d])
        out[row : row + 1, :] = jnp.sum(jnp.where(diagonal, sums, 0.0), axis=0, keepdims=True)


def token_sums(grads, inputs, scale, order, out_order):
    return pl.pallas_call(
        functools.partial(token_sums_kernel, order, out_order),
        out_shape=jax.ShapeDtypeStruct((grads.shape[0], LANES), F32),
        compiler_params=params(6),
        cost_estimate=cost(10**7, 4 * grads.size),
        name="token_sums",
    )(grads, inputs, scale)


def input_grad(order, grads, inputs, words, scale, gain, out, scaled, normed, factor):
    rows, width = inputs.shape
    features = width // len(order)
    place = {device: i for i, device in enumerate(order)}
    words_t = words[...].T
    column = jnp.broadcast_to(scale[...], (LANES, rows)).T
    total = jnp.zeros((rows, LANES), F32)
    for q in range(width // LANES):
        at = slice(q * LANES, (q + 1) * LANES)
        parts = [grads[place[q * LANES // features + h]] for h in range(LANES // features)]
        value = jnp.concatenate(parts, axis=0).astype(F32).T * gain[:, at]
        kept = keep_flags(words_t, q, rows).T * column
        norm = inputs[:, at].astype(F32) * kept
        scaled[:, at] = value
        normed[:, at] = norm
        factor[:, at] = kept
        total += value * norm
    centre = jnp.sum(total, axis=1, keepdims=True) * (1.0 / width)
    for q in range(width // LANES):
        at = slice(q * LANES, (q + 1) * LANES)
        value = factor[:, at] * (scaled[:, at] - normed[:, at] * centre)
        out[:, at] = value.astype(out.dtype)


def middle_kernel(order, parts, grads, inputs, words, scale, gain, copies, out, held, scaled, normed, factor, leave):
    total = jnp.sum(parts[...], axis=0, keepdims=True)
    copies[...] = jnp.broadcast_to(total[:, None, :], copies.shape)

    @pl.when(lax.axis_index("aa") < EARLY)
    def _():
        input_grad(order, grads, inputs, words, scale, gain, held, scaled, normed, factor)
        copy = pltpu.make_async_copy(held, out, leave)
        copy.start()
        copy.wait()


def last_kernel(
    order, norm, parts, grads, inputs, words, scale, gain, _, share, out, held, scaled, normed, factor, leave
):
    share[...] = jnp.sum(parts[...], axis=0)[:, : share.shape[1]] * norm

    @pl.when(lax.axis_index("aa") >= EARLY)
    def _():
        input_grad(order, grads, inputs, words, scale, gain, held, scaled, normed, factor)
        copy = pltpu.make_async_copy(held, out, leave)
        copy.start()
        copy.wait()


def grad_call(kernel, operands, first_out, rows, width, aliased, name):
    vmem, anywhere = pl.BlockSpec(memory_space=pltpu.VMEM), pl.BlockSpec(memory_space=pl.ANY)
    count = len(operands)
    return pl.pallas_call(
        kernel,
        out_shape=(first_out, jax.ShapeDtypeStruct((rows, width), jnp.bfloat16)),
        in_specs=[vmem] * (count - aliased) + [anywhere] * aliased,
        out_specs=(vmem, anywhere),
        scratch_shapes=[pltpu.VMEM((rows, width), jnp.bfloat16)]
        + [pltpu.VMEM((rows, width), F32)] * 3
        + [pltpu.SemaphoreType.DMA],
        input_output_aliases={count - 1: 1} if aliased else {},
        compiler_params=params(14),
        cost_estimate=cost(10**8, 8 * rows * width),
        name=name,
    )(*operands)


def per_device(grad_out, saved_input, keep_bits, gain):
    groups, planes = lax.axis_size("ba"), lax.axis_size("aa")
    features = grad_out.shape[1]
    rows, width = saved_input.shape
    order, sums_order = members(groups, *GRADS_ORDER), members(groups, *SUMS_ORDER)

    pieces, by_device, scale = prepare(grad_out.T, saved_input, keep_bits, order)
    arrived = exchange(pieces, "ba", order)
    sums = token_sums(arrived, by_device, scale, order, sums_order)
    sums = exchange(sums[:, None, :], "ba", sums_order)

    local = (arrived, saved_input, keep_bits, scale, gain.reshape(1, width))
    copies, grad_in = grad_call(
        functools.partial(middle_kernel, order),
        (sums.reshape(groups, LANES), *local),
        jax.ShapeDtypeStruct((planes, 1, LANES), F32),
        rows, width, 0, "middle",
    )
    shares = exchange(copies, "aa", members(planes, *SHARES_ORDER))
    share, grad_in = grad_call(
        functools.partial(last_kernel, order, 1.0 / math.sqrt(rows * groups * planes)),
        (shares, *local, grad_in),
        jax.ShapeDtypeStruct((1, features), F32),
        rows, width, 1, "last",
    )
    return (grad_in, share.reshape(features))


def solution(mesh):
    placed = (P("aa", "ba"), P(("aa", "ba"), None), P(("aa", "ba"), None), P())
    return jax.shard_map(
        per_device,
        mesh=mesh,
        in_specs=placed,
        out_specs=(P(("aa", "ba"), None), P("ba")),
        check_vma=False,
    )
```

```python
import functools
import math

import jax
import jax.numpy as jnp
from jax import lax
from jax.experimental import pallas as pl
from jax.experimental.pallas import tpu as pltpu
from jax.sharding import PartitionSpec as P

KEEP_RATE = 0.9
EPSILON = 1e-06
LANES = 128
BITS = 32
GRADS_ORDER = [(37 + i) % 64 for i in range(64)]
SUMS_ORDER = [(37 + i) % 64 for i in range(64)]
SHARES_ORDER = [(9 + i) % 12 for i in range(12)]
EARLY = 4
F32 = jnp.float32


def exchange(parts, axis, order):
    return lax.all_to_all(parts, axis, 0, 0, tiled=True, axis_index_groups=[order])


def params(mib):
    return pltpu.CompilerParams(vmem_limit_bytes=mib << 20)


def cost(flops, size):
    return pl.CostEstimate(flops=flops, bytes_accessed=size, transcendentals=0)


def keep_flags(words_t, q, rows):
    count = LANES // BITS
    shift = lax.broadcasted_iota(jnp.int32, (count, BITS, rows), 1)
    word = jnp.broadcast_to(words_t[q * count : (q + 1) * count, None, :], (count, BITS, rows))
    return (jnp.right_shift(word, shift) & 1).reshape(LANES, rows).astype(F32)


def prepare_kernel(
    order, grads, inputs, words, pieces, by_device, scale, rows_in, words_in, kept, rows_sem, words_sem, move
):
    rows, width = inputs.shape
    features = width // len(order)
    place = {device: i for i, device in enumerate(order)}
    words_copy = pltpu.make_async_copy(words, words_in, words_sem)
    rows_copy = pltpu.make_async_copy(inputs, rows_in, rows_sem)
    words_copy.start()
    rows_copy.start()
    pl.delay(100)
    for i, device in enumerate(order):
        pltpu.make_async_copy(grads.at[:, pl.ds(device * rows, rows)], pieces.at[i], move).start()
    words_copy.wait()
    words_t = words_in[...].T
    for q in range(width // LANES):
        at = slice(q * LANES, (q + 1) * LANES)
        kept[at, :] = keep_flags(words_t, q, rows).astype(kept.dtype)
    rows_copy.wait()
    squares = jnp.zeros((8, rows), F32)
    for q in range(width // LANES):
        at = slice(q * LANES, (q + 1) * LANES)
        value = rows_in[:, at].T * kept[at, :]
        kept_value = value.astype(F32)
        squares += jnp.sum((kept_value * kept_value).reshape(LANES // 8, 8, rows), axis=0)
        for h in range(LANES // features):
            by_device[place[q * LANES // features + h]] = value[h * features : (h + 1) * features, :]
    mean = jnp.sum(squares, axis=0, keepdims=True) * (1.0 / (KEEP_RATE * KEEP_RATE * width))
    scale[...] = lax.rsqrt(mean + EPSILON) * (1.0 / KEEP_RATE)
    pltpu.make_async_copy(pieces, pieces, move).wait()


def prepare(grads, inputs, words, order):
    rows, width = inputs.shape
    devices = len(order)
    shape = (devices, width // devices, rows)
    return pl.pallas_call(
        functools.partial(prepare_kernel, order),
        out_shape=(
            jax.ShapeDtypeStruct(shape, grads.dtype),
            jax.ShapeDtypeStruct(shape, inputs.dtype),
            jax.ShapeDtypeStruct((1, rows), F32),
        ),
        in_specs=[pl.BlockSpec(memory_space=pltpu.HBM)] * 3,
        scratch_shapes=[
            pltpu.VMEM((rows, width), inputs.dtype),
            pltpu.VMEM(words.shape, words.dtype),
            pltpu.VMEM((width, rows), inputs.dtype),
            pltpu.SemaphoreType.DMA,
            pltpu.SemaphoreType.DMA,
            pltpu.SemaphoreType.DMA,
        ],
        compiler_params=params(6),
        cost_estimate=cost(10**8, 8 * inputs.size),
        name="prepare",
    )(*(pltpu.with_memory_space_constraint(value, pltpu.HBM) for value in (grads, inputs, words)))


def token_sums_kernel(order, out_order, grads, inputs, scale, out):
    devices, features, rows = grads.shape
    shape = (features, LANES)
    diagonal = lax.broadcasted_iota(jnp.int32, shape, 0) == lax.broadcasted_iota(jnp.int32, shape, 1)
    for d in range(devices):
        product = grads[d].astype(F32) * (inputs[d].astype(F32) * scale[...])
        sums = jnp.sum(product, axis=1, keepdims=True)
        row = out_order.index(order[d])
        out[row : row + 1, :] = jnp.sum(jnp.where(diagonal, sums, 0.0), axis=0, keepdims=True)


def token_sums(grads, inputs, scale, order, out_order):
    return pl.pallas_call(
        functools.partial(token_sums_kernel, order, out_order),
        out_shape=jax.ShapeDtypeStruct((grads.shape[0], LANES), F32),
        compiler_params=params(6),
        cost_estimate=cost(10**7, 4 * grads.size),
        name="token_sums",
    )(grads, inputs, scale)


def input_grad(order, grads, inputs, words, scale, gain, out, scaled, normed, factor):
    rows, width = inputs.shape
    features = width // len(order)
    place = {device: i for i, device in enumerate(order)}
    words_t = words[...].T
    column = jnp.broadcast_to(scale[...], (LANES, rows)).T
    total = jnp.zeros((rows, LANES), F32)
    for q in range(width // LANES):
        at = slice(q * LANES, (q + 1) * LANES)
        parts = [grads[place[q * LANES // features + h]] for h in range(LANES // features)]
        value = jnp.concatenate(parts, axis=0).astype(F32).T * gain[:, at]
        kept = keep_flags(words_t, q, rows).T * column
        norm = inputs[:, at].astype(F32) * kept
        scaled[:, at] = value
        normed[:, at] = norm
        factor[:, at] = kept
        total += value * norm
    centre = jnp.sum(total, axis=1, keepdims=True) * (1.0 / width)
    for q in range(width // LANES):
        at = slice(q * LANES, (q + 1) * LANES)
        value = factor[:, at] * (scaled[:, at] - normed[:, at] * centre)
        out[:, at] = value.astype(out.dtype)


def middle_kernel(order, parts, grads, inputs, words, scale, gain, copies, out, held, scaled, normed, factor, leave):
    total = jnp.sum(parts[...], axis=0, keepdims=True)
    copies[...] = jnp.broadcast_to(total[:, None, :], copies.shape)

    @pl.when(lax.axis_index("aa") < EARLY)
    def _():
        input_grad(order, grads, inputs, words, scale, gain, held, scaled, normed, factor)
        copy = pltpu.make_async_copy(held, out, leave)
        copy.start()
        copy.wait()


def last_kernel(
    order, norm, parts, grads, inputs, words, scale, gain, _, share, out, held, scaled, normed, factor, leave
):
    share[...] = jnp.sum(parts[...], axis=0)[:, : share.shape[1]] * norm

    @pl.when(lax.axis_index("aa") >= EARLY)
    def _():
        input_grad(order, grads, inputs, words, scale, gain, held, scaled, normed, factor)
        copy = pltpu.make_async_copy(held, out, leave)
        copy.start()
        copy.wait()


def grad_call(kernel, operands, first_out, rows, width, aliased, name):
    vmem, anywhere = pl.BlockSpec(memory_space=pltpu.VMEM), pl.BlockSpec(memory_space=pl.ANY)
    count = len(operands)
    return pl.pallas_call(
        kernel,
        out_shape=(first_out, jax.ShapeDtypeStruct((rows, width), jnp.bfloat16)),
        in_specs=[vmem] * (count - aliased) + [anywhere] * aliased,
        out_specs=(vmem, anywhere),
        scratch_shapes=[pltpu.VMEM((rows, width), jnp.bfloat16)]
        + [pltpu.VMEM((rows, width), F32)] * 3
        + [pltpu.SemaphoreType.DMA],
        input_output_aliases={count - 1: 1} if aliased else {},
        compiler_params=params(14),
        cost_estimate=cost(10**8, 8 * rows * width),
        name=name,
    )(*operands)


def per_device(grad_out, saved_input, keep_bits, gain):
    groups, planes = lax.axis_size("ba"), lax.axis_size("aa")
    features = grad_out.shape[1]
    rows, width = saved_input.shape
    order, sums_order = GRADS_ORDER, SUMS_ORDER

    pieces, by_device, scale = prepare(grad_out.T, saved_input, keep_bits, order)
    arrived = exchange(pieces, "ba", order)
    sums = token_sums(arrived, by_device, scale, order, sums_order)
    sums = exchange(sums[:, None, :], "ba", sums_order)

    local = (arrived, saved_input, keep_bits, scale, gain.reshape(1, width))
    copies, grad_in = grad_call(
        functools.partial(middle_kernel, order),
        (sums.reshape(groups, LANES), *local),
        jax.ShapeDtypeStruct((planes, 1, LANES), F32),
        rows, width, 0, "middle",
    )
    shares = exchange(copies, "aa", SHARES_ORDER)
    share, grad_in = grad_call(
        functools.partial(last_kernel, order, 1.0 / math.sqrt(rows * groups * planes)),
        (shares, *local, grad_in),
        jax.ShapeDtypeStruct((1, features), F32),
        rows, width, 1, "last",
    )
    return (grad_in, share.reshape(features))


def solution(mesh):
    placed = (P("aa", "ba"), P(("aa", "ba"), None), P(("aa", "ba"), None), P())
    return jax.shard_map(
        per_device,
        mesh=mesh,
        in_specs=placed,
        out_specs=(P(("aa", "ba"), None), P("ba")),
        check_vma=False,
    )
```

```python
import functools
import math

import jax
import jax.numpy as jnp
from jax import lax
from jax.experimental import pallas as pl
from jax.experimental.pallas import tpu as pltpu
from jax.sharding import PartitionSpec as P

KEEP_RATE = 0.9
EPSILON = 1e-06
LANES = 128
BITS = 32
GRADS_ORDER = [(37 + i) % 64 for i in range(64)]
SUMS_ORDER = [(37 + i) % 64 for i in range(64)]
SHARES_ORDER = [(9 + i) % 12 for i in range(12)]
SWAPPED = (3, 4, 5, 6, 7, 9, 10)
CORES = 2
EARLY = 4
F32 = jnp.float32


def exchange(parts, axis, groups):
    return lax.all_to_all(parts, axis, 0, 0, tiled=True, axis_index_groups=groups)


def swaps(plane, device):
    return plane in SWAPPED and device >= CORES


def params(mib):
    return pltpu.CompilerParams(vmem_limit_bytes=mib << 20)


def cost(flops, size):
    return pl.CostEstimate(flops=flops, bytes_accessed=size, transcendentals=0)


def keep_flags(words_t, q, rows):
    count = LANES // BITS
    shift = lax.broadcasted_iota(jnp.int32, (count, BITS, rows), 1)
    word = jnp.broadcast_to(words_t[q * count : (q + 1) * count, None, :], (count, BITS, rows))
    return (jnp.right_shift(word, shift) & 1).reshape(LANES, rows).astype(F32)


def prepare_kernel(
    order, grads, inputs, words, pieces, by_device, scale, rows_in, words_in, kept, rows_sem, words_sem, move
):
    rows, width = inputs.shape
    features = width // len(order)
    place = {device: i for i, device in enumerate(order)}
    words_copy = pltpu.make_async_copy(words, words_in, words_sem)
    rows_copy = pltpu.make_async_copy(inputs, rows_in, rows_sem)
    words_copy.start()
    rows_copy.start()
    pl.delay(100)
    for i, device in enumerate(order):
        pltpu.make_async_copy(grads.at[:, pl.ds(device * rows, rows)], pieces.at[i], move).start()
    words_copy.wait()
    words_t = words_in[...].T
    for q in range(width // LANES):
        at = slice(q * LANES, (q + 1) * LANES)
        kept[at, :] = keep_flags(words_t, q, rows).astype(kept.dtype)
    rows_copy.wait()
    squares = jnp.zeros((8, rows), F32)
    for q in range(width // LANES):
        at = slice(q * LANES, (q + 1) * LANES)
        value = rows_in[:, at].T * kept[at, :]
        kept_value = value.astype(F32)
        squares += jnp.sum((kept_value * kept_value).reshape(LANES // 8, 8, rows), axis=0)
        for h in range(LANES // features):
            by_device[place[q * LANES // features + h]] = value[h * features : (h + 1) * features, :]
    mean = jnp.sum(squares, axis=0, keepdims=True) * (1.0 / (KEEP_RATE * KEEP_RATE * width))
    scale[...] = lax.rsqrt(mean + EPSILON) * (1.0 / KEEP_RATE)
    pltpu.make_async_copy(pieces, pieces, move).wait()


def prepare(grads, inputs, words, order):
    rows, width = inputs.shape
    devices = len(order)
    shape = (devices, width // devices, rows)
    return pl.pallas_call(
        functools.partial(prepare_kernel, order),
        out_shape=(
            jax.ShapeDtypeStruct(shape, grads.dtype),
            jax.ShapeDtypeStruct(shape, inputs.dtype),
            jax.ShapeDtypeStruct((1, rows), F32),
        ),
        in_specs=[pl.BlockSpec(memory_space=pltpu.HBM)] * 3,
        scratch_shapes=[
            pltpu.VMEM((rows, width), inputs.dtype),
            pltpu.VMEM(words.shape, words.dtype),
            pltpu.VMEM((width, rows), inputs.dtype),
            pltpu.SemaphoreType.DMA,
            pltpu.SemaphoreType.DMA,
            pltpu.SemaphoreType.DMA,
        ],
        compiler_params=params(6),
        cost_estimate=cost(10**8, 8 * inputs.size),
        name="prepare",
    )(*(pltpu.with_memory_space_constraint(value, pltpu.HBM) for value in (grads, inputs, words)))


def token_sums_kernel(order, out_order, grads, inputs, scale, out):
    devices, features, rows = grads.shape
    row = lax.broadcasted_iota(jnp.int32, (features, LANES), 0)
    lane = lax.broadcasted_iota(jnp.int32, (features, LANES), 1)
    for first in range(0, devices, CORES):
        chip = jnp.zeros((1, LANES), F32)
        for core in range(CORES):
            d = order.index(first + core)
            product = grads[d].astype(F32) * (inputs[d].astype(F32) * scale[...])
            sums = jnp.sum(product, axis=1, keepdims=True)
            chip += jnp.sum(jnp.where(row == lane - core * features, sums, 0.0), axis=0, keepdims=True)
        for core in range(CORES):
            at = out_order.index(first + core)
            out[at : at + 1, :] = chip


def token_sums(grads, inputs, scale, order, out_order):
    return pl.pallas_call(
        functools.partial(token_sums_kernel, order, out_order),
        out_shape=jax.ShapeDtypeStruct((grads.shape[0], LANES), F32),
        compiler_params=params(6),
        cost_estimate=cost(10**7, 4 * grads.size),
        name="token_sums",
    )(grads, inputs, scale)


def input_grad(order, grads, inputs, words, scale, gain, out, scaled, normed, factor):
    rows, width = inputs.shape
    features = width // len(order)
    place = {device: i for i, device in enumerate(order)}
    words_t = words[...].T
    column = jnp.broadcast_to(scale[...], (LANES, rows)).T
    total = jnp.zeros((rows, LANES), F32)
    for q in range(width // LANES):
        at = slice(q * LANES, (q + 1) * LANES)
        parts = [grads[place[q * LANES // features + h]] for h in range(LANES // features)]
        value = jnp.concatenate(parts, axis=0).astype(F32).T * gain[:, at]
        kept = keep_flags(words_t, q, rows).T * column
        norm = inputs[:, at].astype(F32) * kept
        scaled[:, at] = value
        normed[:, at] = norm
        factor[:, at] = kept
        total += value * norm
    centre = jnp.sum(total, axis=1, keepdims=True) * (1.0 / width)
    for q in range(width // LANES):
        at = slice(q * LANES, (q + 1) * LANES)
        value = factor[:, at] * (scaled[:, at] - normed[:, at] * centre)
        out[:, at] = value.astype(out.dtype)


def middle_kernel(order, parts, grads, inputs, words, scale, gain, copies, out, held, scaled, normed, factor, leave):
    total = jnp.sum(parts[...], axis=0, keepdims=True)
    copies[...] = jnp.broadcast_to(total[:, None, :], copies.shape)

    @pl.when(lax.axis_index("aa") < EARLY)
    def _():
        input_grad(order, grads, inputs, words, scale, gain, held, scaled, normed, factor)
        copy = pltpu.make_async_copy(held, out, leave)
        copy.start()
        copy.wait()


def last_kernel(
    order, norm, parts, grads, inputs, words, scale, gain, _, share, out, held, scaled, normed, factor, leave
):
    total = jnp.sum(parts[...], axis=0) * norm
    features = share.shape[1]
    first, second = total[:, :features], pltpu.roll(total, LANES - features, 1)[:, :features]
    share[...] = jnp.where(lax.axis_index("ba") % CORES == 0, first, second)

    @pl.when(lax.axis_index("aa") >= EARLY)
    def _():
        input_grad(order, grads, inputs, words, scale, gain, held, scaled, normed, factor)
        copy = pltpu.make_async_copy(held, out, leave)
        copy.start()
        copy.wait()


def grad_call(kernel, operands, first_out, rows, width, aliased, name):
    vmem, anywhere = pl.BlockSpec(memory_space=pltpu.VMEM), pl.BlockSpec(memory_space=pl.ANY)
    count = len(operands)
    return pl.pallas_call(
        kernel,
        out_shape=(first_out, jax.ShapeDtypeStruct((rows, width), jnp.bfloat16)),
        in_specs=[vmem] * (count - aliased) + [anywhere] * aliased,
        out_specs=(vmem, anywhere),
        scratch_shapes=[pltpu.VMEM((rows, width), jnp.bfloat16)]
        + [pltpu.VMEM((rows, width), F32)] * 3
        + [pltpu.SemaphoreType.DMA],
        input_output_aliases={count - 1: 1} if aliased else {},
        compiler_params=params(14),
        cost_estimate=cost(10**8, 8 * rows * width),
        name=name,
    )(*operands)


def per_device(grad_out, saved_input, keep_bits, gain):
    groups, planes = lax.axis_size("ba"), lax.axis_size("aa")
    features = grad_out.shape[1]
    rows, width = saved_input.shape
    order, sums_order = GRADS_ORDER, SUMS_ORDER

    pieces, by_device, scale = prepare(grad_out.T, saved_input, keep_bits, order)
    arrived = exchange(pieces, "ba", [order])
    sums = token_sums(arrived, by_device, scale, order, sums_order)
    sums = exchange(sums[:, None, :], "ba", [sums_order])

    local = (arrived, saved_input, keep_bits, scale, gain.reshape(1, width))
    copies, grad_in = grad_call(
        functools.partial(middle_kernel, order),
        (sums.reshape(groups, LANES), *local),
        jax.ShapeDtypeStruct((planes, 1, LANES), F32),
        rows, width, 0, "middle",
    )
    members = [[(z, d + 1 - 2 * (d % CORES) if swaps(z, d) else d) for z in SHARES_ORDER] for d in range(groups)]
    shares = exchange(copies, ("aa", "ba"), [[z * groups + d for z, d in group] for group in members])
    share, grad_in = grad_call(
        functools.partial(last_kernel, order, 1.0 / math.sqrt(rows * groups * planes)),
        (shares, *local, grad_in),
        jax.ShapeDtypeStruct((1, features), F32),
        rows, width, 1, "last",
    )
    return (grad_in, share.reshape(features))


def solution(mesh):
    placed = (P("aa", "ba"), P(("aa", "ba"), None), P(("aa", "ba"), None), P())
    return jax.shard_map(
        per_device,
        mesh=mesh,
        in_specs=placed,
        out_specs=(P(("aa", "ba"), None), P("ba")),
        check_vma=False,
    )
```

```python
import functools
import math

import jax
import jax.numpy as jnp
from jax import lax
from jax.experimental import pallas as pl
from jax.experimental.pallas import tpu as pltpu
from jax.sharding import PartitionSpec as P

KEEP_RATE = 0.9
EPSILON = 1e-06
LANES = 128
BITS = 32
GRADS_ORDER = [(37 + i) % 64 for i in range(64)]
SUMS_ORDER = [(37 + i) % 64 for i in range(64)]
FIRST_PLANES = (9, 8)
SHARES_ORDERS = [[(first + i) % 12 for i in range(12)] for first in FIRST_PLANES]
SWAPPED = (3, 4, 5, 6, 9)
CORES = 2
EARLY = 4
F32 = jnp.float32


def exchange(parts, axis, groups):
    return lax.all_to_all(parts, axis, 0, 0, tiled=True, axis_index_groups=groups)


def swaps(plane, device):
    return plane in SWAPPED and device >= CORES


def params(mib):
    return pltpu.CompilerParams(vmem_limit_bytes=mib << 20)


def cost(flops, size):
    return pl.CostEstimate(flops=flops, bytes_accessed=size, transcendentals=0)


def keep_flags(words_t, q, rows):
    count = LANES // BITS
    shift = lax.broadcasted_iota(jnp.int32, (count, BITS, rows), 1)
    word = jnp.broadcast_to(words_t[q * count : (q + 1) * count, None, :], (count, BITS, rows))
    return (jnp.right_shift(word, shift) & 1).reshape(LANES, rows).astype(F32)


def prepare_kernel(
    order, grads, inputs, words, pieces, by_device, scale, rows_in, words_in, kept, rows_sem, words_sem, move
):
    rows, width = inputs.shape
    features = width // len(order)
    place = {device: i for i, device in enumerate(order)}
    words_copy = pltpu.make_async_copy(words, words_in, words_sem)
    rows_copy = pltpu.make_async_copy(inputs, rows_in, rows_sem)
    words_copy.start()
    rows_copy.start()
    pl.delay(100)
    for i, device in enumerate(order):
        pltpu.make_async_copy(grads.at[:, pl.ds(device * rows, rows)], pieces.at[i], move).start()
    words_copy.wait()
    words_t = words_in[...].T
    for q in range(width // LANES):
        at = slice(q * LANES, (q + 1) * LANES)
        kept[at, :] = keep_flags(words_t, q, rows).astype(kept.dtype)
    rows_copy.wait()
    squares = jnp.zeros((8, rows), F32)
    for q in range(width // LANES):
        at = slice(q * LANES, (q + 1) * LANES)
        value = rows_in[:, at].T * kept[at, :]
        kept_value = value.astype(F32)
        squares += jnp.sum((kept_value * kept_value).reshape(LANES // 8, 8, rows), axis=0)
        for h in range(LANES // features):
            by_device[place[q * LANES // features + h]] = value[h * features : (h + 1) * features, :]
    mean = jnp.sum(squares, axis=0, keepdims=True) * (1.0 / (KEEP_RATE * KEEP_RATE * width))
    scale[...] = lax.rsqrt(mean + EPSILON) * (1.0 / KEEP_RATE)
    pltpu.make_async_copy(pieces, pieces, move).wait()


def prepare(grads, inputs, words, order):
    rows, width = inputs.shape
    devices = len(order)
    shape = (devices, width // devices, rows)
    return pl.pallas_call(
        functools.partial(prepare_kernel, order),
        out_shape=(
            jax.ShapeDtypeStruct(shape, grads.dtype),
            jax.ShapeDtypeStruct(shape, inputs.dtype),
            jax.ShapeDtypeStruct((1, rows), F32),
        ),
        in_specs=[pl.BlockSpec(memory_space=pltpu.HBM)] * 3,
        scratch_shapes=[
            pltpu.VMEM((rows, width), inputs.dtype),
            pltpu.VMEM(words.shape, words.dtype),
            pltpu.VMEM((width, rows), inputs.dtype),
            pltpu.SemaphoreType.DMA,
            pltpu.SemaphoreType.DMA,
            pltpu.SemaphoreType.DMA,
        ],
        compiler_params=params(6),
        cost_estimate=cost(10**8, 8 * inputs.size),
        name="prepare",
    )(*(pltpu.with_memory_space_constraint(value, pltpu.HBM) for value in (grads, inputs, words)))


def token_sums_kernel(order, out_order, grads, inputs, scale, out):
    devices, features, rows = grads.shape
    row = lax.broadcasted_iota(jnp.int32, (features, LANES), 0)
    lane = lax.broadcasted_iota(jnp.int32, (features, LANES), 1)
    for first in range(0, devices, CORES):
        chip = jnp.zeros((1, LANES), F32)
        for core in range(CORES):
            d = order.index(first + core)
            product = grads[d].astype(F32) * (inputs[d].astype(F32) * scale[...])
            sums = jnp.sum(product, axis=1, keepdims=True)
            chip += jnp.sum(jnp.where(row == lane - core * features, sums, 0.0), axis=0, keepdims=True)
        for core in range(CORES):
            at = out_order.index(first + core)
            out[at : at + 1, :] = chip


def token_sums(grads, inputs, scale, order, out_order):
    return pl.pallas_call(
        functools.partial(token_sums_kernel, order, out_order),
        out_shape=jax.ShapeDtypeStruct((grads.shape[0], LANES), F32),
        compiler_params=params(6),
        cost_estimate=cost(10**7, 4 * grads.size),
        name="token_sums",
    )(grads, inputs, scale)


def input_grad(order, grads, inputs, words, scale, gain, out, scaled, normed, factor):
    rows, width = inputs.shape
    features = width // len(order)
    place = {device: i for i, device in enumerate(order)}
    words_t = words[...].T
    column = jnp.broadcast_to(scale[...], (LANES, rows)).T
    total = jnp.zeros((rows, LANES), F32)
    for q in range(width // LANES):
        at = slice(q * LANES, (q + 1) * LANES)
        parts = [grads[place[q * LANES // features + h]] for h in range(LANES // features)]
        value = jnp.concatenate(parts, axis=0).astype(F32).T * gain[:, at]
        kept = keep_flags(words_t, q, rows).T * column
        norm = inputs[:, at].astype(F32) * kept
        scaled[:, at] = value
        normed[:, at] = norm
        factor[:, at] = kept
        total += value * norm
    centre = jnp.sum(total, axis=1, keepdims=True) * (1.0 / width)
    for q in range(width // LANES):
        at = slice(q * LANES, (q + 1) * LANES)
        value = factor[:, at] * (scaled[:, at] - normed[:, at] * centre)
        out[:, at] = value.astype(out.dtype)


def middle_kernel(order, parts, grads, inputs, words, scale, gain, copies, out, held, scaled, normed, factor, leave):
    total = jnp.sum(parts[...], axis=0, keepdims=True)
    copies[...] = jnp.broadcast_to(total[:, None, :], copies.shape)

    @pl.when(lax.axis_index("aa") < EARLY)
    def _():
        input_grad(order, grads, inputs, words, scale, gain, held, scaled, normed, factor)
        copy = pltpu.make_async_copy(held, out, leave)
        copy.start()
        copy.wait()


def last_kernel(
    order, norm, parts, grads, inputs, words, scale, gain, _, share, out, held, scaled, normed, factor, leave
):
    total = jnp.sum(parts[...], axis=0) * norm
    features = share.shape[1]
    first, second = total[:, :features], pltpu.roll(total, LANES - features, 1)[:, :features]
    share[...] = jnp.where(lax.axis_index("ba") % CORES == 0, first, second)

    @pl.when(lax.axis_index("aa") >= EARLY)
    def _():
        input_grad(order, grads, inputs, words, scale, gain, held, scaled, normed, factor)
        copy = pltpu.make_async_copy(held, out, leave)
        copy.start()
        copy.wait()


def grad_call(kernel, operands, first_out, rows, width, aliased, name):
    vmem, anywhere = pl.BlockSpec(memory_space=pltpu.VMEM), pl.BlockSpec(memory_space=pl.ANY)
    count = len(operands)
    return pl.pallas_call(
        kernel,
        out_shape=(first_out, jax.ShapeDtypeStruct((rows, width), jnp.bfloat16)),
        in_specs=[vmem] * (count - aliased) + [anywhere] * aliased,
        out_specs=(vmem, anywhere),
        scratch_shapes=[pltpu.VMEM((rows, width), jnp.bfloat16)]
        + [pltpu.VMEM((rows, width), F32)] * 3
        + [pltpu.SemaphoreType.DMA],
        input_output_aliases={count - 1: 1} if aliased else {},
        compiler_params=params(14),
        cost_estimate=cost(10**8, 8 * rows * width),
        name=name,
    )(*operands)


def per_device(grad_out, saved_input, keep_bits, gain):
    groups, planes = lax.axis_size("ba"), lax.axis_size("aa")
    features = grad_out.shape[1]
    rows, width = saved_input.shape
    order, sums_order = GRADS_ORDER, SUMS_ORDER

    pieces, by_device, scale = prepare(grad_out.T, saved_input, keep_bits, order)
    arrived = exchange(pieces, "ba", [order])
    sums = token_sums(arrived, by_device, scale, order, sums_order)
    sums = exchange(sums[:, None, :], "ba", [sums_order])

    local = (arrived, saved_input, keep_bits, scale, gain.reshape(1, width))
    copies, grad_in = grad_call(
        functools.partial(middle_kernel, order),
        (sums.reshape(groups, LANES), *local),
        jax.ShapeDtypeStruct((planes, 1, LANES), F32),
        rows, width, 0, "middle",
    )
    members = [
        [(z, d + 1 - 2 * (d % CORES) if swaps(z, d) else d) for z in SHARES_ORDERS[d % CORES]]
        for d in range(groups)
    ]
    shares = exchange(copies, ("aa", "ba"), [[z * groups + d for z, d in group] for group in members])
    share, grad_in = grad_call(
        functools.partial(last_kernel, order, 1.0 / math.sqrt(rows * groups * planes)),
        (shares, *local, grad_in),
        jax.ShapeDtypeStruct((1, features), F32),
        rows, width, 1, "last",
    )
    return (grad_in, share.reshape(features))


def solution(mesh):
    placed = (P("aa", "ba"), P(("aa", "ba"), None), P(("aa", "ba"), None), P())
    return jax.shard_map(
        per_device,
        mesh=mesh,
        in_specs=placed,
        out_specs=(P(("aa", "ba"), None), P("ba")),
        check_vma=False,
    )
```

```python
import functools
import math

import jax
import jax.numpy as jnp
from jax import lax
from jax.experimental import pallas as pl
from jax.experimental.pallas import tpu as pltpu
from jax.sharding import PartitionSpec as P

KEEP_RATE = 0.9
EPSILON = 1e-06
LANES = 128
BITS = 32
GRADS_ORDER = [(37 + i) % 64 for i in range(64)]
SUMS_ORDER = [(37 + i) % 64 for i in range(64)]
FIRST_PLANES = (9, 8)
SHARES_ORDERS = [[(first + i) % 12 for i in range(12)] for first in FIRST_PLANES]
SWAPPED = (3, 4, 5, 6, 9)
CORES = 2
EARLY = 4
F32 = jnp.float32


def exchange(parts, axis, groups):
    return lax.all_to_all(parts, axis, 0, 0, tiled=True, axis_index_groups=groups)


def swaps(plane, device):
    return plane in SWAPPED and device >= CORES


def params(mib):
    return pltpu.CompilerParams(vmem_limit_bytes=mib << 20)


def cost(flops, size):
    return pl.CostEstimate(flops=flops, bytes_accessed=size, transcendentals=0)


def keep_flags(words_t, q, rows):
    count = LANES // BITS
    shift = lax.broadcasted_iota(jnp.int32, (count, BITS, rows), 1)
    word = jnp.broadcast_to(words_t[q * count : (q + 1) * count, None, :], (count, BITS, rows))
    return (jnp.right_shift(word, shift) & 1).reshape(LANES, rows).astype(F32)


def prepare_kernel(
    order, grads, inputs, words, pieces, by_device, scale, rows_in, words_in, kept, rows_sem, words_sem, move
):
    rows, width = inputs.shape
    features = width // len(order)
    place = {device: i for i, device in enumerate(order)}
    words_copy = pltpu.make_async_copy(words, words_in, words_sem)
    rows_copy = pltpu.make_async_copy(inputs, rows_in, rows_sem)
    words_copy.start()
    rows_copy.start()
    pl.delay(100)
    for i, device in enumerate(order):
        pltpu.make_async_copy(grads.at[:, pl.ds(device * rows, rows)], pieces.at[i], move).start()
    words_copy.wait()
    words_t = words_in[...].T
    for q in range(width // LANES):
        at = slice(q * LANES, (q + 1) * LANES)
        kept[at, :] = keep_flags(words_t, q, rows).astype(kept.dtype)
    rows_copy.wait()
    squares = jnp.zeros((8, rows), F32)
    for q in range(width // LANES):
        at = slice(q * LANES, (q + 1) * LANES)
        value = rows_in[:, at].T * kept[at, :]
        kept_value = value.astype(F32)
        squares += jnp.sum((kept_value * kept_value).reshape(LANES // 8, 8, rows), axis=0)
        for h in range(LANES // features):
            by_device[place[q * LANES // features + h]] = value[h * features : (h + 1) * features, :]
    mean = jnp.sum(squares, axis=0, keepdims=True) * (1.0 / (KEEP_RATE * KEEP_RATE * width))
    scale[...] = lax.rsqrt(mean + EPSILON) * (1.0 / KEEP_RATE)
    pltpu.make_async_copy(pieces, pieces, move).wait()


def prepare(grads, inputs, words, order):
    rows, width = inputs.shape
    devices = len(order)
    shape = (devices, width // devices, rows)
    return pl.pallas_call(
        functools.partial(prepare_kernel, order),
        out_shape=(
            jax.ShapeDtypeStruct(shape, grads.dtype),
            jax.ShapeDtypeStruct(shape, inputs.dtype),
            jax.ShapeDtypeStruct((1, rows), F32),
            jax.ShapeDtypeStruct(inputs.shape, inputs.dtype),
            jax.ShapeDtypeStruct(words.shape, words.dtype),
        ),
        in_specs=[pl.BlockSpec(memory_space=pltpu.HBM)] * 3,
        scratch_shapes=[
            pltpu.VMEM((width, rows), inputs.dtype),
            pltpu.SemaphoreType.DMA,
            pltpu.SemaphoreType.DMA,
            pltpu.SemaphoreType.DMA,
        ],
        compiler_params=params(6),
        cost_estimate=cost(10**8, 8 * inputs.size),
        name="prepare",
    )(*(pltpu.with_memory_space_constraint(value, pltpu.HBM) for value in (grads, inputs, words)))


def token_sums_kernel(order, out_order, grads, inputs, scale, out):
    devices, features, rows = grads.shape
    row = lax.broadcasted_iota(jnp.int32, (features, LANES), 0)
    lane = lax.broadcasted_iota(jnp.int32, (features, LANES), 1)
    for first in range(0, devices, CORES):
        chip = jnp.zeros((1, LANES), F32)
        for core in range(CORES):
            d = order.index(first + core)
            product = grads[d].astype(F32) * (inputs[d].astype(F32) * scale[...])
            sums = jnp.sum(product, axis=1, keepdims=True)
            chip += jnp.sum(jnp.where(row == lane - core * features, sums, 0.0), axis=0, keepdims=True)
        for core in range(CORES):
            at = out_order.index(first + core)
            out[at : at + 1, :] = chip


def token_sums(grads, inputs, scale, order, out_order):
    return pl.pallas_call(
        functools.partial(token_sums_kernel, order, out_order),
        out_shape=jax.ShapeDtypeStruct((grads.shape[0], LANES), F32),
        compiler_params=params(6),
        cost_estimate=cost(10**7, 4 * grads.size),
        name="token_sums",
    )(grads, inputs, scale)


def input_grad(order, grads, inputs, words, scale, gain, out, scaled, normed, factor):
    rows, width = inputs.shape
    features = width // len(order)
    place = {device: i for i, device in enumerate(order)}
    words_t = words[...].T
    column = jnp.broadcast_to(scale[...], (LANES, rows)).T
    total = jnp.zeros((rows, LANES), F32)
    for q in range(width // LANES):
        at = slice(q * LANES, (q + 1) * LANES)
        parts = [grads[place[q * LANES // features + h]] for h in range(LANES // features)]
        value = jnp.concatenate(parts, axis=0).astype(F32).T * gain[:, at]
        kept = keep_flags(words_t, q, rows).T * column
        norm = inputs[:, at].astype(F32) * kept
        scaled[:, at] = value
        normed[:, at] = norm
        factor[:, at] = kept
        total += value * norm
    centre = jnp.sum(total, axis=1, keepdims=True) * (1.0 / width)
    for q in range(width // LANES):
        at = slice(q * LANES, (q + 1) * LANES)
        value = factor[:, at] * (scaled[:, at] - normed[:, at] * centre)
        out[:, at] = value.astype(out.dtype)


def middle_kernel(order, parts, grads, inputs, words, scale, gain, copies, out, held, scaled, normed, factor, leave):
    total = jnp.sum(parts[...], axis=0, keepdims=True)
    copies[...] = jnp.broadcast_to(total[:, None, :], copies.shape)

    @pl.when(lax.axis_index("aa") < EARLY)
    def _():
        input_grad(order, grads, inputs, words, scale, gain, held, scaled, normed, factor)
        copy = pltpu.make_async_copy(held, out, leave)
        copy.start()
        copy.wait()


def last_kernel(
    order, norm, parts, grads, inputs, words, scale, gain, _, share, out, held, scaled, normed, factor, leave
):
    total = jnp.sum(parts[...], axis=0) * norm
    features = share.shape[1]
    first, second = total[:, :features], pltpu.roll(total, LANES - features, 1)[:, :features]
    share[...] = jnp.where(lax.axis_index("ba") % CORES == 0, first, second)

    @pl.when(lax.axis_index("aa") >= EARLY)
    def _():
        input_grad(order, grads, inputs, words, scale, gain, held, scaled, normed, factor)
        copy = pltpu.make_async_copy(held, out, leave)
        copy.start()
        copy.wait()


def grad_call(kernel, operands, first_out, rows, width, aliased, name):
    vmem, anywhere = pl.BlockSpec(memory_space=pltpu.VMEM), pl.BlockSpec(memory_space=pl.ANY)
    count = len(operands)
    return pl.pallas_call(
        kernel,
        out_shape=(first_out, jax.ShapeDtypeStruct((rows, width), jnp.bfloat16)),
        in_specs=[vmem] * (count - aliased) + [anywhere] * aliased,
        out_specs=(vmem, anywhere),
        scratch_shapes=[pltpu.VMEM((rows, width), jnp.bfloat16)]
        + [pltpu.VMEM((rows, width), F32)] * 3
        + [pltpu.SemaphoreType.DMA],
        input_output_aliases={count - 1: 1} if aliased else {},
        compiler_params=params(14),
        cost_estimate=cost(10**8, 8 * rows * width),
        name=name,
    )(*operands)


def per_device(grad_out, saved_input, keep_bits, gain):
    groups, planes = lax.axis_size("ba"), lax.axis_size("aa")
    features = grad_out.shape[1]
    rows, width = saved_input.shape
    order, sums_order = GRADS_ORDER, SUMS_ORDER

    pieces, by_device, scale, inputs, words = prepare(grad_out.T, saved_input, keep_bits, order)
    arrived = exchange(pieces, "ba", [order])
    sums = token_sums(arrived, by_device, scale, order, sums_order)
    sums = exchange(sums[:, None, :], "ba", [sums_order])

    local = (arrived, inputs, words, scale, gain.reshape(1, width))
    copies, grad_in = grad_call(
        functools.partial(middle_kernel, order),
        (sums.reshape(groups, LANES), *local),
        jax.ShapeDtypeStruct((planes, 1, LANES), F32),
        rows, width, 0, "middle",
    )
    members = [
        [(z, d + 1 - 2 * (d % CORES) if swaps(z, d) else d) for z in SHARES_ORDERS[d % CORES]]
        for d in range(groups)
    ]
    shares = exchange(copies, ("aa", "ba"), [[z * groups + d for z, d in group] for group in members])
    share, grad_in = grad_call(
        functools.partial(last_kernel, order, 1.0 / math.sqrt(rows * groups * planes)),
        (shares, *local, grad_in),
        jax.ShapeDtypeStruct((1, features), F32),
        rows, width, 1, "last",
    )
    return (grad_in, share.reshape(features))


def solution(mesh):
    placed = (P("aa", "ba"), P(("aa", "ba"), None), P(("aa", "ba"), None), P())
    return jax.shard_map(
        per_device,
        mesh=mesh,
        in_specs=placed,
        out_specs=(P(("aa", "ba"), None), P("ba")),
        check_vma=False,
    )
```

```python
import functools
import math

import jax
import jax.numpy as jnp
from jax import lax
from jax.experimental import pallas as pl
from jax.experimental.pallas import tpu as pltpu
from jax.sharding import PartitionSpec as P

KEEP_RATE = 0.9
EPSILON = 1e-06
LANES = 128
BITS = 32
GRADS_ORDER = [(37 + i) % 64 for i in range(64)]
SUMS_ORDER = [(37 + i) % 64 for i in range(64)]
FIRST_PLANES = (9, 8)
SHARES_ORDERS = [[(first + i) % 12 for i in range(12)] for first in FIRST_PLANES]
SWAPPED = (3, 4, 5, 6, 9)
CORES = 2
EARLY = 3
F32 = jnp.float32


def exchange(parts, axis, groups):
    return lax.all_to_all(parts, axis, 0, 0, tiled=True, axis_index_groups=groups)


def swaps(plane, device):
    return plane in SWAPPED and device >= CORES


def params(mib):
    return pltpu.CompilerParams(vmem_limit_bytes=mib << 20)


def cost(flops, size):
    return pl.CostEstimate(flops=flops, bytes_accessed=size, transcendentals=0)


def keep_flags(words_t, q, rows):
    count = LANES // BITS
    shift = lax.broadcasted_iota(jnp.int32, (count, BITS, rows), 1)
    word = jnp.broadcast_to(words_t[q * count : (q + 1) * count, None, :], (count, BITS, rows))
    return (jnp.right_shift(word, shift) & 1).reshape(LANES, rows).astype(F32)


def prepare_kernel(
    order, grads, inputs, words, pieces, by_device, scale, rows_in, words_in, kept, rows_sem, words_sem, move
):
    rows, width = inputs.shape
    features = width // len(order)
    place = {device: i for i, device in enumerate(order)}
    words_copy = pltpu.make_async_copy(words, words_in, words_sem)
    rows_copy = pltpu.make_async_copy(inputs, rows_in, rows_sem)
    words_copy.start()
    rows_copy.start()
    pl.delay(100)
    for i, device in enumerate(order):
        pltpu.make_async_copy(grads.at[:, pl.ds(device * rows, rows)], pieces.at[i], move).start()
    words_copy.wait()
    words_t = words_in[...].T
    for q in range(width // LANES):
        at = slice(q * LANES, (q + 1) * LANES)
        kept[at, :] = keep_flags(words_t, q, rows).astype(kept.dtype)
    rows_copy.wait()
    squares = jnp.zeros((8, rows), F32)
    for q in range(width // LANES):
        at = slice(q * LANES, (q + 1) * LANES)
        value = rows_in[:, at].T * kept[at, :]
        kept_value = value.astype(F32)
        squares += jnp.sum((kept_value * kept_value).reshape(LANES // 8, 8, rows), axis=0)
        for h in range(LANES // features):
            by_device[place[q * LANES // features + h]] = value[h * features : (h + 1) * features, :]
    mean = jnp.sum(squares, axis=0, keepdims=True) * (1.0 / (KEEP_RATE * KEEP_RATE * width))
    scale[...] = lax.rsqrt(mean + EPSILON) * (1.0 / KEEP_RATE)
    pltpu.make_async_copy(pieces, pieces, move).wait()


def prepare(grads, inputs, words, order):
    rows, width = inputs.shape
    devices = len(order)
    shape = (devices, width // devices, rows)
    return pl.pallas_call(
        functools.partial(prepare_kernel, order),
        out_shape=(
            jax.ShapeDtypeStruct(shape, grads.dtype),
            jax.ShapeDtypeStruct(shape, inputs.dtype),
            jax.ShapeDtypeStruct((1, rows), F32),
            jax.ShapeDtypeStruct(inputs.shape, inputs.dtype),
            jax.ShapeDtypeStruct(words.shape, words.dtype),
        ),
        in_specs=[pl.BlockSpec(memory_space=pltpu.HBM)] * 3,
        scratch_shapes=[
            pltpu.VMEM((width, rows), inputs.dtype),
            pltpu.SemaphoreType.DMA,
            pltpu.SemaphoreType.DMA,
            pltpu.SemaphoreType.DMA,
        ],
        compiler_params=params(6),
        cost_estimate=cost(10**8, 8 * inputs.size),
        name="prepare",
    )(*(pltpu.with_memory_space_constraint(value, pltpu.HBM) for value in (grads, inputs, words)))


def token_sums_kernel(order, out_order, grads, inputs, scale, out):
    devices, features, rows = grads.shape
    row = lax.broadcasted_iota(jnp.int32, (features, LANES), 0)
    lane = lax.broadcasted_iota(jnp.int32, (features, LANES), 1)
    for first in range(0, devices, CORES):
        chip = jnp.zeros((1, LANES), F32)
        for core in range(CORES):
            d = order.index(first + core)
            product = grads[d].astype(F32) * (inputs[d].astype(F32) * scale[...])
            sums = jnp.sum(product, axis=1, keepdims=True)
            chip += jnp.sum(jnp.where(row == lane - core * features, sums, 0.0), axis=0, keepdims=True)
        for core in range(CORES):
            at = out_order.index(first + core)
            out[at : at + 1, :] = chip


def token_sums(grads, inputs, scale, order, out_order):
    return pl.pallas_call(
        functools.partial(token_sums_kernel, order, out_order),
        out_shape=jax.ShapeDtypeStruct((grads.shape[0], LANES), F32),
        compiler_params=params(6),
        cost_estimate=cost(10**7, 4 * grads.size),
        name="token_sums",
    )(grads, inputs, scale)


def input_grad(order, grads, inputs, words, scale, gain, out, scaled, normed, factor):
    rows, width = inputs.shape
    features = width // len(order)
    place = {device: i for i, device in enumerate(order)}
    words_t = words[...].T
    column = jnp.broadcast_to(scale[...], (LANES, rows)).T
    total = jnp.zeros((rows, LANES), F32)
    for q in range(width // LANES):
        at = slice(q * LANES, (q + 1) * LANES)
        parts = [grads[place[q * LANES // features + h]] for h in range(LANES // features)]
        value = jnp.concatenate(parts, axis=0).astype(F32).T * gain[:, at]
        kept = keep_flags(words_t, q, rows).T * column
        norm = inputs[:, at].astype(F32) * kept
        scaled[:, at] = value
        normed[:, at] = norm
        factor[:, at] = kept
        total += value * norm
    centre = jnp.sum(total, axis=1, keepdims=True) * (1.0 / width)
    for q in range(width // LANES):
        at = slice(q * LANES, (q + 1) * LANES)
        value = factor[:, at] * (scaled[:, at] - normed[:, at] * centre)
        out[:, at] = value.astype(out.dtype)


def middle_kernel(order, parts, grads, inputs, words, scale, gain, copies, out, held, scaled, normed, factor, leave):
    total = jnp.sum(parts[...], axis=0, keepdims=True)
    copies[...] = jnp.broadcast_to(total[:, None, :], copies.shape)

    @pl.when(lax.axis_index("aa") < EARLY)
    def _():
        input_grad(order, grads, inputs, words, scale, gain, held, scaled, normed, factor)
        copy = pltpu.make_async_copy(held, out, leave)
        copy.start()
        copy.wait()


def last_kernel(
    order, norm, parts, grads, inputs, words, scale, gain, _, share, out, held, scaled, normed, factor, leave, mine, sem
):
    total = jnp.sum(parts[...], axis=0) * norm
    features = share.shape[1]
    first, second = total[:, :features], pltpu.roll(total, LANES - features, 1)[:, :features]
    mine[...] = jnp.where(lax.axis_index("ba") % CORES == 0, first, second)
    share_copy = pltpu.make_async_copy(mine, share, sem)
    share_copy.start()

    @pl.when(lax.axis_index("aa") >= EARLY)
    def _():
        input_grad(order, grads, inputs, words, scale, gain, held, scaled, normed, factor)
        copy = pltpu.make_async_copy(held, out, leave)
        copy.start()
        copy.wait()

    share_copy.wait()


def grad_call(kernel, operands, first_out, rows, width, aliased, name):
    vmem, anywhere = pl.BlockSpec(memory_space=pltpu.VMEM), pl.BlockSpec(memory_space=pl.ANY)
    count = len(operands)
    return pl.pallas_call(
        kernel,
        out_shape=(first_out, jax.ShapeDtypeStruct((rows, width), jnp.bfloat16)),
        in_specs=[vmem] * (count - aliased) + [anywhere] * aliased,
        out_specs=(anywhere if aliased else vmem, anywhere),
        scratch_shapes=[pltpu.VMEM((rows, width), jnp.bfloat16)]
        + [pltpu.VMEM((rows, width), F32)] * 3
        + [pltpu.SemaphoreType.DMA]
        + ([pltpu.VMEM(first_out.shape, F32), pltpu.SemaphoreType.DMA] if aliased else []),
        input_output_aliases={count - 1: 1} if aliased else {},
        compiler_params=params(14),
        cost_estimate=cost(10**8, 8 * rows * width),
        name=name,
    )(*operands)


def per_device(grad_out, saved_input, keep_bits, gain):
    groups, planes = lax.axis_size("ba"), lax.axis_size("aa")
    features = grad_out.shape[1]
    rows, width = saved_input.shape
    order, sums_order = GRADS_ORDER, SUMS_ORDER

    pieces, by_device, scale, inputs, words = prepare(grad_out.T, saved_input, keep_bits, order)
    arrived = exchange(pieces, "ba", [order])
    sums = token_sums(arrived, by_device, scale, order, sums_order)
    sums = exchange(sums[:, None, :], "ba", [sums_order])

    local = (arrived, inputs, words, scale, gain.reshape(1, width))
    copies, grad_in = grad_call(
        functools.partial(middle_kernel, order),
        (sums.reshape(groups, LANES), *local),
        jax.ShapeDtypeStruct((planes, 1, LANES), F32),
        rows, width, 0, "middle",
    )
    members = [
        [(z, d + 1 - 2 * (d % CORES) if swaps(z, d) else d) for z in SHARES_ORDERS[d % CORES]]
        for d in range(groups)
    ]
    shares = exchange(copies, ("aa", "ba"), [[z * groups + d for z, d in group] for group in members])
    share, grad_in = grad_call(
        functools.partial(last_kernel, order, 1.0 / math.sqrt(rows * groups * planes)),
        (shares, *local, grad_in),
        jax.ShapeDtypeStruct((1, features), F32),
        rows, width, 1, "last",
    )
    return (grad_in, share.reshape(features))


def solution(mesh):
    placed = (P("aa", "ba"), P(("aa", "ba"), None), P(("aa", "ba"), None), P())
    return jax.shard_map(
        per_device,
        mesh=mesh,
        in_specs=placed,
        out_specs=(P(("aa", "ba"), None), P("ba")),
        check_vma=False,
    )
```
